8 devices in a mesh: dp: 1 (over z), sp: 8 (over y, x, core).
Axes of the slice: x: 2, y: 2, z: 1, core: 2. Of those that a mesh axis runs over, the one named last changes fastest.
Arguments:
- tokens: bfloat16 [65536, 1024], P(('dp', 'sp'))
- w_q: bfloat16 [1024, 1024], replicated
- w_k: bfloat16 [1024, 1024], replicated
- w_v: bfloat16 [1024, 1024], replicated
- w_o: bfloat16 [1024, 1024], replicated
- grad_y: bfloat16 [65536, 1024], P(('dp', 'sp'))
Outputs:
- output 1: bfloat16 [65536, 1024], P(('dp', 'sp'))
- output 2: bfloat16 [65536, 1024], P(('dp', 'sp'))
- output 3: float32 [1024, 1024], P('dp')
- output 4: float32 [1024, 1024], P('dp')
- output 5: float32 [1024, 1024], P('dp')
- output 6: float32 [1024, 1024], P('dp')
All inputs are finite; a program needn't handle non-finite values.
Results may differ from the reference program's by a relative error of at most 0.00355113.
Values are sent between devices in bfloat16 or wider.
A program may use at most 1 GiB of HBM per device.

```python
import math
import jax
import jax.numpy as jnp

SEQ_LEN = 65536
MODEL_DIM = 1024
HEAD_DIM = 128
BLOCK_LEN = 128


def setup_inputs(seed: int = 0, part: int = 0) -> dict:
    part_key = jax.random.fold_in(jax.random.key(seed), part)
    key_x, key_dy = jax.random.split(part_key)
    key_q, key_k, key_v, key_o = jax.random.split(jax.random.key(seed + 1), 4)
    w_scale = MODEL_DIM ** -0.5
    shape_w = (MODEL_DIM, MODEL_DIM)

    def normal_weight(key_w):
        return (jax.random.normal(key_w, shape_w, jnp.float32) * w_scale).astype(jnp.bfloat16)

    tokens = jax.random.normal(key_x, (SEQ_LEN, MODEL_DIM), jnp.float32)
    grad_y = jax.random.normal(key_dy, (SEQ_LEN, MODEL_DIM), jnp.float32) * SEQ_LEN ** -0.25
    return {"tokens": tokens.astype(jnp.bfloat16), "w_q": normal_weight(key_q), "w_k": normal_weight(key_k), "w_v": normal_weight(key_v), "w_o": normal_weight(key_o), "grad_y": grad_y.astype(jnp.bfloat16)}


def reference(tokens, w_q, w_k, w_v, w_o, grad_y):
    n_heads = MODEL_DIM // HEAD_DIM
    n_blocks = SEQ_LEN // BLOCK_LEN
    att_scale = 1.0 / math.sqrt(SEQ_LEN * HEAD_DIM)
    causal = jnp.arange(BLOCK_LEN)[:, None] >= jnp.arange(BLOCK_LEN)[None, :]

    def project(operand, weight):
        return jnp.dot(operand, weight, preferred_element_type=jnp.float32).astype(jnp.bfloat16)

    def split_heads(tensor):
        return tensor.reshape(n_blocks, BLOCK_LEN, n_heads, HEAD_DIM).astype(jnp.float32)

    def to_rows(tensor):
        return (tensor * att_scale).astype(jnp.bfloat16).reshape(SEQ_LEN, MODEL_DIM)

    def as_bf16(tensor):
        return tensor.astype(jnp.bfloat16).astype(jnp.float32)

    def excl_prefix(blocks):
        zero_block = jnp.zeros_like(blocks[:1])
        return jnp.concatenate([zero_block, jnp.cumsum(blocks, axis=0)[:-1]], axis=0)

    q_heads = split_heads(project(tokens, w_q))
    k_heads = split_heads(project(tokens, w_k))
    v_heads = split_heads(project(tokens, w_v))
    fwd_state = as_bf16(excl_prefix(jnp.einsum("nshd,nshe->nhde", k_heads, v_heads)))
    masked_scores = as_bf16(jnp.where(causal, jnp.einsum("nthd,nshd->nhts", q_heads, k_heads), 0.0))
    out_rows = to_rows(jnp.einsum("nhts,nshe->nthe", masked_scores, v_heads) + jnp.einsum("nthd,nhde->nthe", q_heads, fwd_state))
    out_y = project(out_rows, w_o)

    do_heads = split_heads(project(grad_y, w_o.T))
    block_qdo = jnp.einsum("nthd,nthe->nhde", q_heads, do_heads)
    rev_state = as_bf16(excl_prefix(block_qdo[::-1])[::-1])
    masked_grads = as_bf16(jnp.where(causal, jnp.einsum("nthe,nshe->nhts", do_heads, v_heads), 0.0))
    dq_rows = to_rows(jnp.einsum("nhts,nshd->nthd", masked_grads, k_heads) + jnp.einsum("nthe,nhde->nthd", do_heads, fwd_state))
    dk_rows = to_rows(jnp.einsum("nhts,nthd->nshd", masked_grads, q_heads) + jnp.einsum("nshe,nhde->nshd", v_heads, rev_state))
    dv_rows = to_rows(jnp.einsum("nhts,nthe->nshe", masked_scores, do_heads) + jnp.einsum("nshd,nhde->nshe", k_heads, rev_state))
    grad_x = (jnp.dot(dq_rows, w_q.T, preferred_element_type=jnp.float32) + jnp.dot(dk_rows, w_k.T, preferred_element_type=jnp.float32) + jnp.dot(dv_rows, w_v.T, preferred_element_type=jnp.float32)).astype(jnp.bfloat16)
    grad_wq = jnp.dot(tokens.T, dq_rows, preferred_element_type=jnp.float32)
    grad_wk = jnp.dot(tokens.T, dk_rows, preferred_element_type=jnp.float32)
    grad_wv = jnp.dot(tokens.T, dv_rows, preferred_element_type=jnp.float32)
    grad_wo = jnp.dot(out_rows.T, grad_y, preferred_element_type=jnp.float32)
    return (out_y, grad_x, grad_wq, grad_wk, grad_wv, grad_wo)
```

```python
import functools
import math
import jax
import jax.numpy as jnp
from jax import lax
from jax.experimental import pallas as pl
from jax.experimental.pallas import tpu as pltpu
from jax.sharding import PartitionSpec as P

HEAD_DIM = 128
BLOCK_LEN = 128
GROUPS = 2

F32 = jnp.float32
BF16 = jnp.bfloat16


def dot_nn(a, b):
    return jnp.dot(a, b, preferred_element_type=F32)


def dot_nt(a, b):
    return lax.dot_general(a, b, (((1,), (1,)), ((), ())), preferred_element_type=F32)


def dot_tn(a, b):
    return lax.dot_general(a, b, (((0,), (0,)), ((), ())), preferred_element_type=F32)


def proj_kernel(x_ref, dy_ref, wq_ref, wk_ref, wv_ref, wo_ref, q_ref, k_ref, v_ref, g_ref, tot_ref):
    @pl.when(pl.program_id(0) == 0)
    def _():
        tot_ref[...] = jnp.zeros_like(tot_ref)

    q_ref[...] = dot_nn(x_ref[...], wq_ref[...]).astype(BF16)
    k_ref[...] = dot_nn(x_ref[...], wk_ref[...]).astype(BF16)
    v_ref[...] = dot_nn(x_ref[...], wv_ref[...]).astype(BF16)
    g_ref[...] = dot_nt(dy_ref[...], wo_ref[...]).astype(BF16)
    for h in range(tot_ref.shape[1]):
        cols = slice(h * HEAD_DIM, (h + 1) * HEAD_DIM)
        tot_ref[0, h] += dot_tn(k_ref[:, cols], v_ref[:, cols])
        tot_ref[1, h] += dot_tn(q_ref[:, cols], g_ref[:, cols])


def project(tokens, grad_y, w_q, w_k, w_v, w_o, group, tile):
    n_rows, dim = tokens.shape
    cols = dim // GROUPS
    heads = cols // HEAD_DIM
    row_in = pl.BlockSpec((tile, dim), lambda i: (i, 0))
    w_in = pl.BlockSpec((dim, cols), lambda i: (0, group))
    row_out = pl.BlockSpec((tile, cols), lambda i: (i, 0))
    rows = jax.ShapeDtypeStruct((n_rows, cols), BF16)
    return pl.pallas_call(
        proj_kernel,
        grid=(n_rows // tile,),
        in_specs=[row_in, row_in, w_in, w_in, w_in, pl.BlockSpec((cols, dim), lambda i: (group, 0))],
        out_specs=[row_out] * 4 + [pl.BlockSpec((2, heads, HEAD_DIM, HEAD_DIM), lambda i: (0, 0, 0, 0))],
        out_shape=[rows] * 4 + [jax.ShapeDtypeStruct((2, heads, HEAD_DIM, HEAD_DIM), F32)],
        cost_estimate=pl.CostEstimate(flops=8 * n_rows * dim * cols, bytes_accessed=2 * n_rows * (2 * dim + 4 * cols), transcendentals=0),
        name=f"project{group}",
    )(tokens, grad_y, w_q, w_k, w_v, w_o)


def attn_kernel(scale, q_ref, k_ref, v_ref, g_ref, tot_ref, o_ref, dq_ref, dk_ref, dv_ref, s_ref, r_ref, a_ref, at_ref, c_ref, ct_ref, sb_ref, st_ref, rb_ref, rt_ref):
    n_heads = s_ref.shape[0]

    @pl.when(pl.program_id(0) == 0)
    def _():
        me = lax.axis_index("sp")
        for h in range(n_heads):
            s_ref[h] = jnp.zeros_like(s_ref[h])
            r_ref[h] = jnp.zeros_like(r_ref[h])
            for d in range(tot_ref.shape[0]):
                s_ref[h] += jnp.where(d < me, tot_ref[d, 0, h], 0.0)
                r_ref[h] += jnp.where(d >= me, tot_ref[d, 1, h], 0.0)

    causal = lax.broadcasted_iota(jnp.int32, (BLOCK_LEN, BLOCK_LEN), 0) >= lax.broadcasted_iota(jnp.int32, (BLOCK_LEN, BLOCK_LEN), 1)
    units = [(b, h) for b in range(q_ref.shape[0] // BLOCK_LEN) for h in range(n_heads)]

    def load(b, h):
        rows = slice(b * BLOCK_LEN, (b + 1) * BLOCK_LEN)
        cols = slice(h * HEAD_DIM, (h + 1) * HEAD_DIM)
        return rows, cols, q_ref[rows, cols], k_ref[rows, cols], v_ref[rows, cols], g_ref[rows, cols]

    for i, (b, h) in enumerate(units):
        _, _, q, k, v, g = load(b, h)
        kt = k.T
        a = jnp.where(causal, dot_nn(q, kt), 0.0).astype(BF16)
        c = jnp.where(causal, dot_nn(g, v.T), 0.0).astype(BF16)
        a_ref[i] = a
        c_ref[i] = c
        at_ref[i] = a.T
        ct_ref[i] = c.T
        s = s_ref[h]
        r = r_ref[h] - dot_nn(q.T, g)
        s_ref[h] = s + dot_nn(kt, v)
        r_ref[h] = r
        s = s.astype(BF16)
        r = r.astype(BF16)
        sb_ref[i] = s
        st_ref[i] = s.T
        rb_ref[i] = r
        rt_ref[i] = r.T

    def pair(left, left_state, right, right_state):
        return dot_nn(jnp.concatenate([left, left_state], axis=1), jnp.concatenate([right, right_state], axis=0)) * scale

    for i, (b, h) in enumerate(units):
        rows, cols, q, k, v, g = load(b, h)
        o_ref[rows, cols] = pair(a_ref[i], q, v, sb_ref[i]).astype(BF16)
        dq_ref[rows, cols] = pair(c_ref[i], g, k, st_ref[i]).astype(BF16)
        dk_ref[rows, cols] = pair(ct_ref[i], v, q, rt_ref[i]).astype(BF16)
        dv_ref[rows, cols] = pair(at_ref[i], k, g, rb_ref[i]).astype(BF16)


def attend(q, k, v, g, totals, scale, group, tile):
    n_rows, cols = q.shape
    heads = cols // HEAD_DIM
    row_spec = pl.BlockSpec((tile, cols), lambda i: (i, 0))
    state = (heads, HEAD_DIM, HEAD_DIM)
    units = (tile // BLOCK_LEN * heads, BLOCK_LEN, BLOCK_LEN)
    return pl.pallas_call(
        functools.partial(attn_kernel, scale),
        grid=(n_rows // tile,),
        in_specs=[row_spec] * 4 + [pl.BlockSpec(totals.shape, lambda i: (0, 0, 0, 0, 0))],
        out_specs=[row_spec] * 4,
        out_shape=[jax.ShapeDtypeStruct((n_rows, cols), BF16)] * 4,
        scratch_shapes=[pltpu.VMEM(state, F32)] * 2 + [pltpu.VMEM(units, BF16)] * 8,
        cost_estimate=pl.CostEstimate(flops=64 * n_rows * cols * HEAD_DIM, bytes_accessed=16 * n_rows * cols, transcendentals=0),
        name=f"attend{group}",
    )(q, k, v, g, totals)


def wgrad_kernel(x_ref, dy_ref, o_ref, dq_ref, dk_ref, dv_ref, grad_ref):
    @pl.when(pl.program_id(0) == 0)
    def _():
        grad_ref[...] = jnp.zeros_like(grad_ref)

    xt = x_ref[...].T
    grad_ref[0] += dot_nn(xt, dq_ref[...])
    grad_ref[1] += dot_nn(xt, dk_ref[...])
    grad_ref[2] += dot_nn(xt, dv_ref[...])
    cols = o_ref.shape[1]
    grad_o = dot_tn(o_ref[...], dy_ref[...])
    for part in range(GROUPS):
        grad_ref[3, part * cols:(part + 1) * cols] += grad_o[:, part * cols:(part + 1) * cols]


def weight_grads(tokens, grad_y, o, dq, dk, dv, group, tile):
    n_rows, dim = tokens.shape
    cols = o.shape[1]
    wide = pl.BlockSpec((tile, dim), lambda i: (i, 0))
    half = pl.BlockSpec((tile, cols), lambda i: (i, 0))
    return pl.pallas_call(
        wgrad_kernel,
        grid=(n_rows // tile,),
        in_specs=[wide, wide] + [half] * 4,
        out_specs=pl.BlockSpec((4, dim, cols), lambda i: (0, 0, 0)),
        out_shape=jax.ShapeDtypeStruct((4, dim, cols), F32),
        cost_estimate=pl.CostEstimate(flops=8 * n_rows * dim * cols, bytes_accessed=2 * n_rows * (2 * dim + 4 * cols), transcendentals=0),
        name=f"wgrad{group}",
    )(tokens, grad_y, o, dq, dk, dv)


def add_rows(dst, start, src):
    step = 64

    def body(i, carry):
        there = pl.ds(pl.multiple_of(start + i * step, step), step)
        dst[there, :] += src[pl.ds(pl.multiple_of(i * step, step), step), :]
        return carry

    lax.fori_loop(0, src.shape[0] // step, body, 0)


def reduce_kernel(marks, dq0_ref, dq1_ref, dk0_ref, dk1_ref, wq_ref, wk_ref, grad_ref, part_ref, shard_ref, own, got, got_x, got_y, end_x, end_y, send_sem, recv_sem, local_sem):
    step = pl.program_id(0)
    me = lax.axis_index("sp")
    core, x, y = me % 2, (me // 2) % 2, (me // 4) % 2
    peer_core, peer_x, peer_y = me + 1 - 2 * core, me + 2 - 4 * x, me + 4 - 8 * y
    half = own.shape[0]
    quarter, eighth, last = half // 2, half // 4, half // 8

    def rows(ref, start, size):
        return ref.at[pl.ds(pl.multiple_of(start, last), size), :]

    def remote(i, src, dst, peer):
        return pltpu.make_async_remote_copy(src_ref=src, dst_ref=dst, send_sem=send_sem.at[i], recv_sem=recv_sem.at[i], device_id={"sp": peer}, device_id_type=pl.DeviceIdType.MESH)

    keep_x, keep_y = x * eighth, quarter + y * eighth
    swap = remote(0, rows(grad_ref, (1 - core) * half, half), got, peer_core)
    local = pltpu.make_async_copy(rows(grad_ref, core * half, half), own, local_sem)
    first_x = remote(1, rows(own, (1 - x) * eighth, eighth), got_x, peer_x)
    first_y = remote(2, rows(own, quarter + (1 - y) * eighth, eighth), got_y, peer_y)
    second_x = remote(3, rows(own, keep_x + (1 - y) * last, last), end_x, peer_y)
    second_y = remote(4, rows(own, keep_y + (1 - x) * last, last), end_y, peer_x)

    @pl.when(step == 0)
    def _():
        barrier = pltpu.get_barrier_semaphore()
        for peer in (peer_core, peer_x, peer_y):
            pl.semaphore_signal(barrier, inc=1, device_id={"sp": peer}, device_id_type=pl.DeviceIdType.MESH)
        pl.semaphore_wait(barrier, 3)
        swap.start()
        local.start()

    @pl.when(step == marks[0])
    def _():
        local.wait()
        swap.wait()
        add_rows(own, 0, got)

    @pl.when(step == marks[1])
    def _():
        first_x.wait()
        first_y.wait()
        add_rows(own, keep_x, got_x)
        add_rows(own, keep_y, got_y)

    dq = jnp.concatenate([dq0_ref[...], dq1_ref[...]], axis=1)
    dk = jnp.concatenate([dk0_ref[...], dk1_ref[...]], axis=1)
    part_ref[...] = dot_nt(dq, wq_ref[...]) + dot_nt(dk, wk_ref[...])

    @pl.when(step == marks[0])
    def _():
        first_x.start()
        first_y.start()

    @pl.when(step == marks[1])
    def _():
        second_x.start()
        second_y.start()

    @pl.when(step == pl.num_programs(0) - 1)
    def _():
        second_x.wait()
        second_y.wait()
        shard_ref[0] = own[pl.ds(pl.multiple_of(keep_x + y * last, last), last), :] + end_x[...]
        shard_ref[1] = own[pl.ds(pl.multiple_of(keep_y + x * last, last), last), :] + end_y[...]


def reduce_beside(parts, w_q, w_k, grads, tile, marks):
    n_rows, cols = parts[0].shape
    dim = w_q.shape[0]
    total = grads.shape[0] * grads.shape[1]
    half = pl.BlockSpec((tile, cols), lambda i: (i, 0))
    weight = pl.BlockSpec((dim, dim), lambda i: (0, 0))
    shard = (2, total // 16, cols)
    sizes = [total // 2, total // 2, total // 8, total // 8, total // 16, total // 16]
    return pl.pallas_call(
        functools.partial(reduce_kernel, marks),
        grid=(n_rows // tile,),
        in_specs=[half] * 4 + [weight] * 2 + [pl.BlockSpec(memory_space=pl.ANY)],
        out_specs=[pl.BlockSpec((tile, dim), lambda i: (i, 0)), pl.BlockSpec(shard, lambda i: (0, 0, 0))],
        out_shape=[jax.ShapeDtypeStruct((n_rows, dim), F32), jax.ShapeDtypeStruct(shard, F32)],
        scratch_shapes=[pltpu.VMEM((size, cols), F32) for size in sizes] + [pltpu.SemaphoreType.DMA((5,))] * 2 + [pltpu.SemaphoreType.DMA],
        compiler_params=pltpu.CompilerParams(collective_id=0, has_side_effects=True),
        cost_estimate=pl.CostEstimate(flops=4 * n_rows * dim * dim, bytes_accessed=8 * n_rows * dim, transcendentals=0),
        name="reduce_beside",
    )(*parts, w_q, w_k, grads.reshape(total, cols))


def out_kernel(o0_ref, o1_ref, dv0_ref, dv1_ref, part_ref, wo_ref, wv_ref, grad_ref, y_ref, dx_ref, gq_ref, gk_ref, gv_ref, go_ref):
    y_ref[...] = dot_nn(jnp.concatenate([o0_ref[...], o1_ref[...]], axis=1), wo_ref[...]).astype(BF16)
    dv = jnp.concatenate([dv0_ref[...], dv1_ref[...]], axis=1)
    dx_ref[...] = (part_ref[...] + dot_nt(dv, wv_ref[...])).astype(BF16)
    for i, ref in enumerate((gq_ref, gk_ref, gv_ref, go_ref)):
        ref[...] = grad_ref[i]


def back_project(parts, partial, w_o, w_v, grads, tile):
    n_rows, cols = parts[0].shape
    dim = w_o.shape[1]
    steps = n_rows // tile
    piece = dim // steps
    down = cols // piece
    half = pl.BlockSpec((tile, cols), lambda i: (i, 0))
    weight = pl.BlockSpec((dim, dim), lambda i: (0, 0))
    row_out = pl.BlockSpec((tile, dim), lambda i: (i, 0))
    left = pl.BlockSpec((piece, cols), lambda i: (i, 0))
    return pl.pallas_call(
        out_kernel,
        grid=(steps,),
        in_specs=[half] * 4 + [row_out] + [weight] * 2 + [pl.BlockSpec((4, piece, cols), lambda i: (0, i, 0))],
        out_specs=[row_out] * 2 + [left] * 3 + [pl.BlockSpec((piece, cols), lambda i: (i % down, i // down))],
        out_shape=[jax.ShapeDtypeStruct((n_rows, dim), BF16)] * 2 + [jax.ShapeDtypeStruct((dim, dim), F32)] * 4,
        cost_estimate=pl.CostEstimate(flops=4 * n_rows * dim * dim, bytes_accessed=12 * n_rows * dim, transcendentals=0),
        name="back_project",
    )(*parts, partial, w_o, w_v, grads)


def place_kernel(s0_ref, s1_ref, s2_ref, s3_ref, a0_ref, a1_ref, a2_ref, a3_ref, gq_ref, gk_ref, gv_ref, go_ref):
    for src, dst in ((s0_ref, gq_ref), (s1_ref, gk_ref), (s2_ref, gv_ref), (s3_ref, go_ref)):
        dst[...] = src[0, 0]


def place(gathered, grads):
    piece, cols = gathered.shape[2:]
    down = cols // piece

    def source(slot):
        if slot % 2:
            return lambda i: (i * 2 + slot // 2, 1, 0, 0)
        return lambda i: (((i % 2) * 2 + i // 2) * 2 + slot // 2, 0, 0, 0)

    right = pl.BlockSpec((piece, cols), lambda i: (i, 1))
    return pl.pallas_call(
        place_kernel,
        grid=(4,),
        in_specs=[pl.BlockSpec((1, 1, piece, cols), source(slot)) for slot in range(4)] + [pl.BlockSpec(memory_space=pl.ANY)] * 4,
        out_specs=[right] * 3 + [pl.BlockSpec((piece, cols), lambda i: (down + i % down, i // down))],
        out_shape=[jax.ShapeDtypeStruct(g.shape, g.dtype) for g in grads],
        input_output_aliases={4 + i: i for i in range(4)},
        cost_estimate=pl.CostEstimate(flops=0, bytes_accessed=8 * gathered.size, transcendentals=0),
        name="place",
    )(*[gathered] * 4, *grads)


def solution(mesh):
    n_seq = mesh.shape["sp"]
    row_spec = P(("dp", "sp"), None)
    grad_spec = P("dp", None)

    def local_layer(tokens, w_q, w_k, w_v, w_o, grad_y):
        scale = 1.0 / math.sqrt(tokens.shape[0] * n_seq * HEAD_DIM)
        projected = [project(tokens, grad_y, w_q, w_k, w_v, w_o, g, 1024) for g in range(GROUPS)]
        gathered = [lax.all_gather(p[4], "sp") for p in projected]
        parts = [None] * GROUPS
        parts[0] = attend(*projected[0][:4], gathered[0], scale, 0, 512)
        first = lax.psum(weight_grads(tokens, grad_y, *parts[0], 0, 1024), "sp")
        parts[1] = attend(*projected[1][:4], gathered[1], scale, 1, 512)
        second = weight_grads(tokens, grad_y, *parts[1], 1, 1024)
        o, dq, dk, dv = zip(*parts)
        partial, shard = reduce_beside(dq + dk, w_q, w_k, second, 512, (3, 13))
        shards = lax.all_gather(shard, "sp")
        out_y, grad_x, *grads = back_project(o + dv, partial, w_o, w_v, first, 512)
        return (out_y, grad_x) + tuple(place(shards, grads))

    return jax.shard_map(local_layer, mesh=mesh, in_specs=(row_spec, P(), P(), P(), P(), row_spec), out_specs=(row_spec, row_spec, grad_spec, grad_spec, grad_spec, grad_spec), check_vma=False)
```

```python
import functools
import math
import jax
import jax.numpy as jnp
from jax import lax
from jax.experimental import pallas as pl
from jax.experimental.pallas import tpu as pltpu
from jax.sharding import PartitionSpec as P

HEAD_DIM = 128
BLOCK_LEN = 128
GROUPS = 2
MARKS = ((2, 0, 0), (4, 1, 0), (8, 0, 1), (13, 1, 1))

F32 = jnp.float32
BF16 = jnp.bfloat16


def dot_nn(a, b):
    return jnp.dot(a, b, preferred_element_type=F32)


def dot_nt(a, b):
    return lax.dot_general(a, b, (((1,), (1,)), ((), ())), preferred_element_type=F32)


def dot_tn(a, b):
    return lax.dot_general(a, b, (((0,), (0,)), ((), ())), preferred_element_type=F32)


def proj_kernel(x_ref, dy_ref, wq_ref, wk_ref, wv_ref, wo_ref, q_ref, k_ref, v_ref, g_ref, tot_ref):
    @pl.when(pl.program_id(0) == 0)
    def _():
        tot_ref[...] = jnp.zeros_like(tot_ref)

    q_ref[...] = dot_nn(x_ref[...], wq_ref[...]).astype(BF16)
    k_ref[...] = dot_nn(x_ref[...], wk_ref[...]).astype(BF16)
    v_ref[...] = dot_nn(x_ref[...], wv_ref[...]).astype(BF16)
    g_ref[...] = dot_nt(dy_ref[...], wo_ref[...]).astype(BF16)
    for h in range(tot_ref.shape[1]):
        cols = slice(h * HEAD_DIM, (h + 1) * HEAD_DIM)
        tot_ref[0, h] += dot_tn(k_ref[:, cols], v_ref[:, cols])
        tot_ref[1, h] += dot_tn(q_ref[:, cols], g_ref[:, cols])


def project(tokens, grad_y, w_q, w_k, w_v, w_o, group, tile):
    n_rows, dim = tokens.shape
    cols = dim // GROUPS
    heads = cols // HEAD_DIM
    row_in = pl.BlockSpec((tile, dim), lambda i: (i, 0))
    w_in = pl.BlockSpec((dim, cols), lambda i: (0, group))
    row_out = pl.BlockSpec((tile, cols), lambda i: (i, 0))
    rows = jax.ShapeDtypeStruct((n_rows, cols), BF16)
    return pl.pallas_call(
        proj_kernel,
        grid=(n_rows // tile,),
        in_specs=[row_in, row_in, w_in, w_in, w_in, pl.BlockSpec((cols, dim), lambda i: (group, 0))],
        out_specs=[row_out] * 4 + [pl.BlockSpec((2, heads, HEAD_DIM, HEAD_DIM), lambda i: (0, 0, 0, 0))],
        out_shape=[rows] * 4 + [jax.ShapeDtypeStruct((2, heads, HEAD_DIM, HEAD_DIM), F32)],
        cost_estimate=pl.CostEstimate(flops=8 * n_rows * dim * cols, bytes_accessed=2 * n_rows * (2 * dim + 4 * cols), transcendentals=0),
        name=f"project{group}",
    )(tokens, grad_y, w_q, w_k, w_v, w_o)


def attn_kernel(scale, q_ref, k_ref, v_ref, g_ref, tot_ref, o_ref, dq_ref, dk_ref, dv_ref, s_ref, r_ref, a_ref, at_ref, c_ref, ct_ref, sb_ref, st_ref, rb_ref, rt_ref):
    n_heads = s_ref.shape[0]

    @pl.when(pl.program_id(0) == 0)
    def _():
        me = lax.axis_index("sp")
        for h in range(n_heads):
            s_ref[h] = jnp.zeros_like(s_ref[h])
            r_ref[h] = jnp.zeros_like(r_ref[h])
            for d in range(tot_ref.shape[0]):
                s_ref[h] += jnp.where(d < me, tot_ref[d, 0, h], 0.0)
                r_ref[h] += jnp.where(d >= me, tot_ref[d, 1, h], 0.0)

    causal = lax.broadcasted_iota(jnp.int32, (BLOCK_LEN, BLOCK_LEN), 0) >= lax.broadcasted_iota(jnp.int32, (BLOCK_LEN, BLOCK_LEN), 1)
    units = [(b, h) for b in range(q_ref.shape[0] // BLOCK_LEN) for h in range(n_heads)]

    def load(b, h):
        rows = slice(b * BLOCK_LEN, (b + 1) * BLOCK_LEN)
        cols = slice(h * HEAD_DIM, (h + 1) * HEAD_DIM)
        return rows, cols, q_ref[rows, cols], k_ref[rows, cols], v_ref[rows, cols], g_ref[rows, cols]

    for i, (b, h) in enumerate(units):
        _, _, q, k, v, g = load(b, h)
        kt = k.T
        a = jnp.where(causal, dot_nn(q, kt), 0.0).astype(BF16)
        c = jnp.where(causal, dot_nn(g, v.T), 0.0).astype(BF16)
        a_ref[i] = a
        c_ref[i] = c
        at_ref[i] = a.T
        ct_ref[i] = c.T
        s = s_ref[h]
        r = r_ref[h] - dot_nn(q.T, g)
        s_ref[h] = s + dot_nn(kt, v)
        r_ref[h] = r
        s = s.astype(BF16)
        r = r.astype(BF16)
        sb_ref[i] = s
        st_ref[i] = s.T
        rb_ref[i] = r
        rt_ref[i] = r.T

    def pair(left, left_state, right, right_state):
        return dot_nn(jnp.concatenate([left, left_state], axis=1), jnp.concatenate([right, right_state], axis=0)) * scale

    for i, (b, h) in enumerate(units):
        rows, cols, q, k, v, g = load(b, h)
        o_ref[rows, cols] = pair(a_ref[i], q, v, sb_ref[i]).astype(BF16)
        dq_ref[rows, cols] = pair(c_ref[i], g, k, st_ref[i]).astype(BF16)
        dk_ref[rows, cols] = pair(ct_ref[i], v, q, rt_ref[i]).astype(BF16)
        dv_ref[rows, cols] = pair(at_ref[i], k, g, rb_ref[i]).astype(BF16)


def attend_scatter_kernel(scale, marks, q_ref, k_ref, v_ref, g_ref, tot_ref, grad_ref, o_ref, dq_ref, dk_ref, dv_ref, shard_ref, *scratch):
    def compute():
        attn_kernel(scale, q_ref, k_ref, v_ref, g_ref, tot_ref, o_ref, dq_ref, dk_ref, dv_ref, *scratch[:10])

    scatter_beside(marks, grad_ref, shard_ref, *scratch[10:], compute)


def attend(q, k, v, g, totals, scale, group, tile, grads=None, marks=None):
    n_rows, cols = q.shape
    heads = cols // HEAD_DIM
    row_spec = pl.BlockSpec((tile, cols), lambda i: (i, 0))
    state = (heads, HEAD_DIM, HEAD_DIM)
    units = (tile // BLOCK_LEN * heads, BLOCK_LEN, BLOCK_LEN)
    body = functools.partial(attn_kernel, scale)
    in_specs = [row_spec] * 4 + [pl.BlockSpec(totals.shape, lambda i: (0, 0, 0, 0, 0))]
    out_specs = [row_spec] * 4
    out_shape = [jax.ShapeDtypeStruct((n_rows, cols), BF16)] * 4
    scratch_shapes = [pltpu.VMEM(state, F32)] * 2 + [pltpu.VMEM(units, BF16)] * 8
    operands = [q, k, v, g, totals]
    params = None
    if grads is not None:
        total = grads.shape[0] * grads.shape[1]
        shard = shard_shape(total, cols)
        body = functools.partial(attend_scatter_kernel, scale, marks)
        in_specs.append(pl.BlockSpec(memory_space=pl.ANY))
        out_specs.append(pl.BlockSpec(shard, lambda i: (0, 0, 0, 0)))
        out_shape.append(jax.ShapeDtypeStruct(shard, F32))
        scratch_shapes += scatter_scratch(total, cols)
        operands.append(grads.reshape(total, cols))
        params = pltpu.CompilerParams(collective_id=1, has_side_effects=True)
    return pl.pallas_call(
        body,
        grid=(n_rows // tile,),
        in_specs=in_specs,
        out_specs=out_specs,
        out_shape=out_shape,
        scratch_shapes=scratch_shapes,
        compiler_params=params,
        cost_estimate=pl.CostEstimate(flops=64 * n_rows * cols * HEAD_DIM, bytes_accessed=16 * n_rows * cols, transcendentals=0),
        name=f"attend{group}",
    )(*operands)


def wgrad_kernel(x_ref, dy_ref, o_ref, dq_ref, dk_ref, dv_ref, grad_ref):
    @pl.when(pl.program_id(0) == 0)
    def _():
        grad_ref[...] = jnp.zeros_like(grad_ref)

    xt = x_ref[...].T
    grad_ref[0] += dot_nn(xt, dq_ref[...])
    grad_ref[1] += dot_nn(xt, dk_ref[...])
    grad_ref[2] += dot_nn(xt, dv_ref[...])
    cols = o_ref.shape[1]
    grad_o = dot_tn(o_ref[...], dy_ref[...])
    for part in range(GROUPS):
        grad_ref[3, part * cols:(part + 1) * cols] += grad_o[:, part * cols:(part + 1) * cols]


def weight_grads(tokens, grad_y, o, dq, dk, dv, group, tile):
    n_rows, dim = tokens.shape
    cols = o.shape[1]
    wide = pl.BlockSpec((tile, dim), lambda i: (i, 0))
    half = pl.BlockSpec((tile, cols), lambda i: (i, 0))
    return pl.pallas_call(
        wgrad_kernel,
        grid=(n_rows // tile,),
        in_specs=[wide, wide] + [half] * 4,
        out_specs=pl.BlockSpec((4, dim, cols), lambda i: (0, 0, 0)),
        out_shape=jax.ShapeDtypeStruct((4, dim, cols), F32),
        cost_estimate=pl.CostEstimate(flops=8 * n_rows * dim * cols, bytes_accessed=2 * n_rows * (2 * dim + 4 * cols), transcendentals=0),
        name=f"wgrad{group}",
    )(tokens, grad_y, o, dq, dk, dv)


def add_rows(dst, start, src):
    step = 64

    def body(i, carry):
        there = pl.ds(pl.multiple_of(start + i * step, step), step)
        dst[there, :] += src[pl.ds(pl.multiple_of(i * step, step), step), :]
        return carry

    lax.fori_loop(0, src.shape[0] // step, body, 0)


CHUNKS = 2


def scatter_scratch(total, cols):
    piece = total // CHUNKS
    sizes = [piece // part for part in (2, 2, 8, 8, 16, 16) for _ in range(CHUNKS)]
    return [pltpu.VMEM((size, cols), F32) for size in sizes] + [pltpu.SemaphoreType.DMA((5 * CHUNKS,))] * 2 + [pltpu.SemaphoreType.DMA((CHUNKS,))]


def shard_shape(total, cols):
    return CHUNKS, 2, total // CHUNKS // 16, cols


def scatter_beside(marks, grad_ref, shard_ref, *rest):
    scratch, (send_sem, recv_sem, local_sem, compute) = rest[:-4], rest[-4:]
    own, got, got_x, got_y, end_x, end_y = (scratch[i * CHUNKS:(i + 1) * CHUNKS] for i in range(6))
    step = pl.program_id(0)
    me = lax.axis_index("sp")
    core, x, y = me % 2, (me // 2) % 2, (me // 4) % 2
    peer_core, peer_x, peer_y = me + 1 - 2 * core, me + 2 - 4 * x, me + 4 - 8 * y
    half = own[0].shape[0]
    quarter, eighth, last = half // 2, half // 4, half // 8
    keep_x, keep_y = x * eighth, quarter + y * eighth

    def rows(ref, start, size):
        return ref.at[pl.ds(pl.multiple_of(start, last), size), :]

    def remote(i, src, dst, peer):
        return pltpu.make_async_remote_copy(src_ref=src, dst_ref=dst, send_sem=send_sem.at[i], recv_sem=recv_sem.at[i], device_id={"sp": peer}, device_id_type=pl.DeviceIdType.MESH)

    def local(c):
        return pltpu.make_async_copy(rows(grad_ref, (2 * c + core) * half, half), own[c], local_sem.at[c])

    def copies(c, hop):
        if hop == 0:
            return (remote(5 * c, rows(grad_ref, (2 * c + 1 - core) * half, half), got[c], peer_core),)
        if hop == 1:
            return (remote(5 * c + 1, rows(own[c], (1 - x) * eighth, eighth), got_x[c], peer_x),
                    remote(5 * c + 2, rows(own[c], quarter + (1 - y) * eighth, eighth), got_y[c], peer_y))
        return (remote(5 * c + 3, rows(own[c], keep_x + (1 - y) * last, last), end_x[c], peer_y),
                remote(5 * c + 4, rows(own[c], keep_y + (1 - x) * last, last), end_y[c], peer_x))

    def start(c, hop):
        for copy in copies(c, hop):
            copy.start()

    def finish(c, hop):
        if hop == 0:
            local(c).wait()
        for copy in copies(c, hop):
            copy.wait()
        if hop == 0:
            add_rows(own[c], 0, got[c])
        elif hop == 1:
            add_rows(own[c], keep_x, got_x[c])
            add_rows(own[c], keep_y, got_y[c])
        else:
            for i, (at, end) in enumerate(((keep_x + y * last, end_x[c]), (keep_y + x * last, end_y[c]))):
                shard_ref[c, i] = own[c][pl.ds(pl.multiple_of(at, last), last), :] + end[...]

    def go_on(c, hop):
        if hop == 0 and c + 1 < CHUNKS:
            start(c + 1, 0)
        if hop < 2:
            start(c, hop + 1)

    @pl.when(step == 0)
    def _():
        barrier = pltpu.get_barrier_semaphore()
        for peer in (peer_core, peer_x, peer_y):
            pl.semaphore_signal(barrier, inc=1, device_id={"sp": peer}, device_id_type=pl.DeviceIdType.MESH)
        pl.semaphore_wait(barrier, 3)
        start(0, 0)
        for c in range(CHUNKS):
            local(c).start()

    for at, c, hop in marks:
        pl.when(step == at)(functools.partial(finish, c, hop))

    compute()

    for at, c, hop in marks:
        pl.when(step == at)(functools.partial(go_on, c, hop))

    @pl.when(step == pl.num_programs(0) - 1)
    def _():
        met = [mark[1:] for mark in marks]
        for hop in (1, 2):
            for c in range(CHUNKS):
                if (c, hop) not in met:
                    finish(c, hop)
                    go_on(c, hop)


def reduce_kernel(marks, dq0_ref, dq1_ref, dk0_ref, dk1_ref, wq_ref, wk_ref, grad_ref, part_ref, shard_ref, *scratch):
    def compute():
        dq = jnp.concatenate([dq0_ref[...], dq1_ref[...]], axis=1)
        dk = jnp.concatenate([dk0_ref[...], dk1_ref[...]], axis=1)
        part_ref[...] = dot_nt(dq, wq_ref[...]) + dot_nt(dk, wk_ref[...])

    scatter_beside(marks, grad_ref, shard_ref, *scratch, compute)


def reduce_beside(parts, w_q, w_k, grads, tile, marks):
    n_rows, cols = parts[0].shape
    dim = w_q.shape[0]
    total = grads.shape[0] * grads.shape[1]
    half = pl.BlockSpec((tile, cols), lambda i: (i, 0))
    weight = pl.BlockSpec((dim, dim), lambda i: (0, 0))
    shard = shard_shape(total, cols)
    return pl.pallas_call(
        functools.partial(reduce_kernel, marks),
        grid=(n_rows // tile,),
        in_specs=[half] * 4 + [weight] * 2 + [pl.BlockSpec(memory_space=pl.ANY)],
        out_specs=[pl.BlockSpec((tile, dim), lambda i: (i, 0)), pl.BlockSpec(shard, lambda i: (0, 0, 0, 0))],
        out_shape=[jax.ShapeDtypeStruct((n_rows, dim), F32), jax.ShapeDtypeStruct(shard, F32)],
        scratch_shapes=scatter_scratch(total, cols),
        compiler_params=pltpu.CompilerParams(collective_id=0, has_side_effects=True),
        cost_estimate=pl.CostEstimate(flops=4 * n_rows * dim * dim, bytes_accessed=8 * n_rows * dim, transcendentals=0),
        name="reduce_beside",
    )(*parts, w_q, w_k, grads.reshape(total, cols))


def shard_specs(rows, cols, per_piece):
    def source(slot):
        def index(i):
            piece = i // per_piece
            part, hi, lo = piece // 4, (piece // 2) % 2, piece % 2
            x = hi + part * (lo - hi)
            y = lo + part * (hi - lo)
            return (y * 2 + x) * 2 + slot % 2, slot // 2, part, i % per_piece, 0
        return index

    return [pl.BlockSpec((1, 1, 1, rows, cols), source(slot)) for slot in range(4)]


def grad_specs(rows, cols, group):
    down = cols // rows
    return [pl.BlockSpec((rows, cols), lambda i: (i, group))] * 3 + [pl.BlockSpec((rows, cols), lambda i: (group * down + i % down, i // down))]


def out_kernel(o0_ref, o1_ref, dv0_ref, dv1_ref, part_ref, wo_ref, wv_ref, s0_ref, s1_ref, s2_ref, s3_ref, y_ref, dx_ref, gq_ref, gk_ref, gv_ref, go_ref):
    y_ref[...] = dot_nn(jnp.concatenate([o0_ref[...], o1_ref[...]], axis=1), wo_ref[...]).astype(BF16)
    dv = jnp.concatenate([dv0_ref[...], dv1_ref[...]], axis=1)
    dx_ref[...] = (part_ref[...] + dot_nt(dv, wv_ref[...])).astype(BF16)
    for src, dst in ((s0_ref, gq_ref), (s1_ref, gk_ref), (s2_ref, gv_ref), (s3_ref, go_ref)):
        dst[...] = src[0, 0, 0]


def back_project(parts, partial, w_o, w_v, gathered, tile):
    n_rows, cols = parts[0].shape
    dim = w_o.shape[1]
    steps = n_rows // tile
    piece = dim // steps
    half = pl.BlockSpec((tile, cols), lambda i: (i, 0))
    weight = pl.BlockSpec((dim, dim), lambda i: (0, 0))
    row_out = pl.BlockSpec((tile, dim), lambda i: (i, 0))
    return pl.pallas_call(
        out_kernel,
        grid=(steps,),
        in_specs=[half] * 4 + [row_out] + [weight] * 2 + shard_specs(piece, cols, steps // 8),
        out_specs=[row_out] * 2 + grad_specs(piece, cols, 0),
        out_shape=[jax.ShapeDtypeStruct((n_rows, dim), BF16)] * 2 + [jax.ShapeDtypeStruct((dim, dim), F32)] * 4,
        cost_estimate=pl.CostEstimate(flops=4 * n_rows * dim * dim, bytes_accessed=12 * n_rows * dim, transcendentals=0),
        name="back_project",
    )(*parts, partial, w_o, w_v, *[gathered] * 4)


def place_kernel(s0_ref, s1_ref, s2_ref, s3_ref, a0_ref, a1_ref, a2_ref, a3_ref, gq_ref, gk_ref, gv_ref, go_ref):
    for src, dst in ((s0_ref, gq_ref), (s1_ref, gk_ref), (s2_ref, gv_ref), (s3_ref, go_ref)):
        dst[...] = src[0, 0, 0]


def place(gathered, grads):
    piece, cols = gathered.shape[3:]
    return pl.pallas_call(
        place_kernel,
        grid=(8,),
        in_specs=shard_specs(piece, cols, 1) + [pl.BlockSpec(memory_space=pl.ANY)] * 4,
        out_specs=grad_specs(piece, cols, 1),
        out_shape=[jax.ShapeDtypeStruct(g.shape, g.dtype) for g in grads],
        input_output_aliases={4 + i: i for i in range(4)},
        cost_estimate=pl.CostEstimate(flops=0, bytes_accessed=8 * gathered.size, transcendentals=0),
        name="place",
    )(*[gathered] * 4, *grads)


def solution(mesh):
    n_seq = mesh.shape["sp"]
    row_spec = P(("dp", "sp"), None)
    grad_spec = P("dp", None)

    def local_layer(tokens, w_q, w_k, w_v, w_o, grad_y):
        scale = 1.0 / math.sqrt(tokens.shape[0] * n_seq * HEAD_DIM)
        projected = [project(tokens, grad_y, w_q, w_k, w_v, w_o, g, 1024) for g in range(GROUPS)]
        gathered = [lax.all_gather(p[4], "sp") for p in projected]
        parts = [None] * GROUPS
        parts[0] = attend(*projected[0][:4], gathered[0], scale, 0, 512)
        first = weight_grads(tokens, grad_y, *parts[0], 0, 1024)
        *parts[1], shard0 = attend(*projected[1][:4], gathered[1], scale, 1, 512, first, MARKS)
        shards0 = lax.all_gather(shard0, "sp")
        second = weight_grads(tokens, grad_y, *parts[1], 1, 1024)
        o, dq, dk, dv = zip(*parts)
        partial, shard1 = reduce_beside(dq + dk, w_q, w_k, second, 512, MARKS)
        shards1 = lax.all_gather(shard1, "sp")
        out_y, grad_x, *grads = back_project(o + dv, partial, w_o, w_v, shards0, 512)
        return (out_y, grad_x) + tuple(place(shards1, grads))

    return jax.shard_map(local_layer, mesh=mesh, in_specs=(row_spec, P(), P(), P(), P(), row_spec), out_specs=(row_spec, row_spec, grad_spec, grad_spec, grad_spec, grad_spec), check_vma=False)
```

```python
import functools
import math
import jax
import jax.numpy as jnp
from jax import lax
from jax.experimental import pallas as pl
from jax.experimental.pallas import tpu as pltpu
from jax.sharding import PartitionSpec as P

HEAD_DIM = 128
BLOCK_LEN = 128
GROUPS = 2
MARKS = ((2, 0, 0), (5, 1, 0), (8, 0, 1), (13, 1, 1))

F32 = jnp.float32
BF16 = jnp.bfloat16


def dot_nn(a, b):
    return jnp.dot(a, b, preferred_element_type=F32)


def dot_nt(a, b):
    return lax.dot_general(a, b, (((1,), (1,)), ((), ())), preferred_element_type=F32)


def dot_tn(a, b):
    return lax.dot_general(a, b, (((0,), (0,)), ((), ())), preferred_element_type=F32)


def proj_kernel(x_ref, dy_ref, wq_ref, wk_ref, wv_ref, wo_ref, q_ref, k_ref, v_ref, g_ref, tot_ref):
    @pl.when(pl.program_id(0) == 0)
    def _():
        tot_ref[...] = jnp.zeros_like(tot_ref)

    q_ref[...] = dot_nn(x_ref[...], wq_ref[...]).astype(BF16)
    k_ref[...] = dot_nn(x_ref[...], wk_ref[...]).astype(BF16)
    v_ref[...] = dot_nn(x_ref[...], wv_ref[...]).astype(BF16)
    g_ref[...] = dot_nt(dy_ref[...], wo_ref[...]).astype(BF16)
    for h in range(tot_ref.shape[1]):
        cols = slice(h * HEAD_DIM, (h + 1) * HEAD_DIM)
        tot_ref[0, h] += dot_tn(k_ref[:, cols], v_ref[:, cols])
        tot_ref[1, h] += dot_tn(q_ref[:, cols], g_ref[:, cols])


def project(tokens, grad_y, w_q, w_k, w_v, w_o, group, tile):
    n_rows, dim = tokens.shape
    cols = dim // GROUPS
    heads = cols // HEAD_DIM
    row_in = pl.BlockSpec((tile, dim), lambda i: (i, 0))
    w_in = pl.BlockSpec((dim, cols), lambda i: (0, group))
    row_out = pl.BlockSpec((tile, cols), lambda i: (i, 0))
    rows = jax.ShapeDtypeStruct((n_rows, cols), BF16)
    return pl.pallas_call(
        proj_kernel,
        grid=(n_rows // tile,),
        in_specs=[row_in, row_in, w_in, w_in, w_in, pl.BlockSpec((cols, dim), lambda i: (group, 0))],
        out_specs=[row_out] * 4 + [pl.BlockSpec((2, heads, HEAD_DIM, HEAD_DIM), lambda i: (0, 0, 0, 0))],
        out_shape=[rows] * 4 + [jax.ShapeDtypeStruct((2, heads, HEAD_DIM, HEAD_DIM), F32)],
        cost_estimate=pl.CostEstimate(flops=8 * n_rows * dim * cols, bytes_accessed=2 * n_rows * (2 * dim + 4 * cols), transcendentals=0),
        name=f"project{group}",
    )(tokens, grad_y, w_q, w_k, w_v, w_o)


def attn_kernel(scale, q_ref, k_ref, v_ref, g_ref, tot_ref, o_ref, dq_ref, dk_ref, dv_ref, s_ref, r_ref, a_ref, at_ref, c_ref, ct_ref, sb_ref, st_ref, rb_ref, rt_ref):
    n_heads = s_ref.shape[0]

    @pl.when(pl.program_id(0) == 0)
    def _():
        me = lax.axis_index("sp")
        for h in range(n_heads):
            s_ref[h] = jnp.zeros_like(s_ref[h])
            r_ref[h] = jnp.zeros_like(r_ref[h])
            for d in range(tot_ref.shape[0]):
                s_ref[h] += jnp.where(d < me, tot_ref[d, 0, h], 0.0)
                r_ref[h] += jnp.where(d >= me, tot_ref[d, 1, h], 0.0)

    causal = lax.broadcasted_iota(jnp.int32, (BLOCK_LEN, BLOCK_LEN), 0) >= lax.broadcasted_iota(jnp.int32, (BLOCK_LEN, BLOCK_LEN), 1)
    units = [(b, h) for b in range(q_ref.shape[0] // BLOCK_LEN) for h in range(n_heads)]

    def load(b, h):
        rows = slice(b * BLOCK_LEN, (b + 1) * BLOCK_LEN)
        cols = slice(h * HEAD_DIM, (h + 1) * HEAD_DIM)
        return rows, cols, q_ref[rows, cols], k_ref[rows, cols], v_ref[rows, cols], g_ref[rows, cols]

    for i, (b, h) in enumerate(units):
        _, _, q, k, v, g = load(b, h)
        kt = k.T
        a = jnp.where(causal, dot_nn(q, kt), 0.0).astype(BF16)
        c = jnp.where(causal, dot_nn(g, v.T), 0.0).astype(BF16)
        a_ref[i] = a
        c_ref[i] = c
        at_ref[i] = a.T
        ct_ref[i] = c.T
        s = s_ref[h]
        r = r_ref[h] - dot_nn(q.T, g)
        s_ref[h] = s + dot_nn(kt, v)
        r_ref[h] = r
        s = s.astype(BF16)
        r = r.astype(BF16)
        sb_ref[i] = s
        st_ref[i] = s.T
        rb_ref[i] = r
        rt_ref[i] = r.T

    def pair(left, left_state, right, right_state):
        return dot_nn(jnp.concatenate([left, left_state], axis=1), jnp.concatenate([right, right_state], axis=0)) * scale

    for i, (b, h) in enumerate(units):
        rows, cols, q, k, v, g = load(b, h)
        o_ref[rows, cols] = pair(a_ref[i], q, v, sb_ref[i]).astype(BF16)
        dq_ref[rows, cols] = pair(c_ref[i], g, k, st_ref[i]).astype(BF16)
        dk_ref[rows, cols] = pair(ct_ref[i], v, q, rt_ref[i]).astype(BF16)
        dv_ref[rows, cols] = pair(at_ref[i], k, g, rb_ref[i]).astype(BF16)


def attend_scatter_kernel(scale, marks, q_ref, k_ref, v_ref, g_ref, tot_ref, grad_ref, o_ref, dq_ref, dk_ref, dv_ref, shard_ref, *scratch):
    def compute():
        attn_kernel(scale, q_ref, k_ref, v_ref, g_ref, tot_ref, o_ref, dq_ref, dk_ref, dv_ref, *scratch[:10])

    scatter_beside(marks, grad_ref, shard_ref, *scratch[10:], compute)


def attend(q, k, v, g, totals, scale, group, tile, grads=None, marks=None):
    n_rows, cols = q.shape
    heads = cols // HEAD_DIM
    row_spec = pl.BlockSpec((tile, cols), lambda i: (i, 0))
    state = (heads, HEAD_DIM, HEAD_DIM)
    units = (tile // BLOCK_LEN * heads, BLOCK_LEN, BLOCK_LEN)
    body = functools.partial(attn_kernel, scale)
    in_specs = [row_spec] * 4 + [pl.BlockSpec(totals.shape, lambda i: (0, 0, 0, 0, 0))]
    out_specs = [row_spec] * 4
    out_shape = [jax.ShapeDtypeStruct((n_rows, cols), BF16)] * 4
    scratch_shapes = [pltpu.VMEM(state, F32)] * 2 + [pltpu.VMEM(units, BF16)] * 8
    operands = [q, k, v, g, totals]
    params = None
    if grads is not None:
        total = grads.shape[0] * grads.shape[1]
        shard = shard_shape(total, cols)
        body = functools.partial(attend_scatter_kernel, scale, marks)
        in_specs.append(pl.BlockSpec(memory_space=pl.ANY))
        out_specs.append(pl.BlockSpec(shard, lambda i: (0, 0, 0, 0)))
        out_shape.append(jax.ShapeDtypeStruct(shard, F32))
        scratch_shapes += scatter_scratch(total, cols)
        operands.append(grads.reshape(total, cols))
        params = pltpu.CompilerParams(collective_id=1, has_side_effects=True)
    return pl.pallas_call(
        body,
        grid=(n_rows // tile,),
        in_specs=in_specs,
        out_specs=out_specs,
        out_shape=out_shape,
        scratch_shapes=scratch_shapes,
        compiler_params=params,
        cost_estimate=pl.CostEstimate(flops=64 * n_rows * cols * HEAD_DIM, bytes_accessed=16 * n_rows * cols, transcendentals=0),
        name=f"attend{group}",
    )(*operands)


def wgrad_kernel(x_ref, dy_ref, o_ref, dq_ref, dk_ref, dv_ref, grad_ref):
    @pl.when(pl.program_id(0) == 0)
    def _():
        grad_ref[...] = jnp.zeros_like(grad_ref)

    xt = x_ref[...].T
    grad_ref[0] += dot_nn(xt, dq_ref[...])
    grad_ref[1] += dot_nn(xt, dk_ref[...])
    grad_ref[2] += dot_nn(xt, dv_ref[...])
    cols = o_ref.shape[1]
    grad_o = dot_tn(o_ref[...], dy_ref[...])
    for part in range(GROUPS):
        grad_ref[3, part * cols:(part + 1) * cols] += grad_o[:, part * cols:(part + 1) * cols]


def weight_grads(tokens, grad_y, o, dq, dk, dv, group, tile):
    n_rows, dim = tokens.shape
    cols = o.shape[1]
    wide = pl.BlockSpec((tile, dim), lambda i: (i, 0))
    half = pl.BlockSpec((tile, cols), lambda i: (i, 0))
    return pl.pallas_call(
        wgrad_kernel,
        grid=(n_rows // tile,),
        in_specs=[wide, wide] + [half] * 4,
        out_specs=pl.BlockSpec((4, dim, cols), lambda i: (0, 0, 0)),
        out_shape=jax.ShapeDtypeStruct((4, dim, cols), F32),
        cost_estimate=pl.CostEstimate(flops=8 * n_rows * dim * cols, bytes_accessed=2 * n_rows * (2 * dim + 4 * cols), transcendentals=0),
        name=f"wgrad{group}",
    )(tokens, grad_y, o, dq, dk, dv)


def add_rows(dst, start, src):
    step = 128

    def body(i, carry):
        there = pl.ds(pl.multiple_of(start + i * step, step), step)
        dst[there, :] += src[pl.ds(pl.multiple_of(i * step, step), step), :]
        return carry

    lax.fori_loop(0, src.shape[0] // step, body, 0)


CHUNKS = 2


def scatter_scratch(total, cols):
    piece = total // CHUNKS
    sizes = [piece // part for part in (2, 2, 8, 8, 16, 16) for _ in range(CHUNKS)]
    return [pltpu.VMEM((size, cols), F32) for size in sizes] + [pltpu.SemaphoreType.DMA((5 * CHUNKS,))] * 2 + [pltpu.SemaphoreType.DMA((CHUNKS,))]


def shard_shape(total, cols):
    return CHUNKS, 2, total // CHUNKS // 16, cols


def scatter_beside(marks, grad_ref, shard_ref, *rest):
    scratch, (send_sem, recv_sem, local_sem, compute) = rest[:-4], rest[-4:]
    own, got, got_x, got_y, end_x, end_y = (scratch[i * CHUNKS:(i + 1) * CHUNKS] for i in range(6))
    step = pl.program_id(0)
    me = lax.axis_index("sp")
    core, x, y = me % 2, (me // 2) % 2, (me // 4) % 2
    peer_core, peer_x, peer_y = me + 1 - 2 * core, me + 2 - 4 * x, me + 4 - 8 * y
    half = own[0].shape[0]
    quarter, eighth, last = half // 2, half // 4, half // 8
    keep_x, keep_y = x * eighth, quarter + y * eighth

    def rows(ref, start, size):
        return ref.at[pl.ds(pl.multiple_of(start, last), size), :]

    def remote(i, src, dst, peer):
        return pltpu.make_async_remote_copy(src_ref=src, dst_ref=dst, send_sem=send_sem.at[i], recv_sem=recv_sem.at[i], device_id={"sp": peer}, device_id_type=pl.DeviceIdType.MESH)

    def local(c):
        return pltpu.make_async_copy(rows(grad_ref, (2 * c + core) * half, half), own[c], local_sem.at[c])

    def copies(c, hop):
        if hop == 0:
            return (remote(5 * c, rows(grad_ref, (2 * c + 1 - core) * half, half), got[c], peer_core),)
        if hop == 1:
            return (remote(5 * c + 1, rows(own[c], (1 - x) * eighth, eighth), got_x[c], peer_x),
                    remote(5 * c + 2, rows(own[c], quarter + (1 - y) * eighth, eighth), got_y[c], peer_y))
        return (remote(5 * c + 3, rows(own[c], keep_x + (1 - y) * last, last), end_x[c], peer_y),
                remote(5 * c + 4, rows(own[c], keep_y + (1 - x) * last, last), end_y[c], peer_x))

    def start(c, hop):
        for copy in copies(c, hop):
            copy.start()

    def finish(c, hop):
        if hop == 0:
            local(c).wait()
        for copy in copies(c, hop):
            copy.wait()
        if hop == 0:
            add_rows(own[c], 0, got[c])
        elif hop == 1:
            add_rows(own[c], keep_x, got_x[c])
            add_rows(own[c], keep_y, got_y[c])
        else:
            for i, (at, end) in enumerate(((keep_x + y * last, end_x[c]), (keep_y + x * last, end_y[c]))):
                shard_ref[c, i] = own[c][pl.ds(pl.multiple_of(at, last), last), :] + end[...]

    def go_on(c, hop):
        if hop == 0 and c + 1 < CHUNKS:
            start(c + 1, 0)
        if hop < 2:
            start(c, hop + 1)

    @pl.when(step == 0)
    def _():
        barrier = pltpu.get_barrier_semaphore()
        for peer in (peer_core, peer_x, peer_y):
            pl.semaphore_signal(barrier, inc=1, device_id={"sp": peer}, device_id_type=pl.DeviceIdType.MESH)
        pl.semaphore_wait(barrier, 3)
        start(0, 0)
        for c in range(CHUNKS):
            local(c).start()

    for at, c, hop in marks:
        pl.when(step == at)(functools.partial(finish, c, hop))

    compute()

    for at, c, hop in marks:
        pl.when(step == at)(functools.partial(go_on, c, hop))

    @pl.when(step == pl.num_programs(0) - 1)
    def _():
        met = [mark[1:] for mark in marks]
        for hop in (1, 2):
            for c in range(CHUNKS):
                if (c, hop) not in met:
                    finish(c, hop)
                    go_on(c, hop)


def reduce_kernel(marks, dq0_ref, dq1_ref, dk0_ref, dk1_ref, wq_ref, wk_ref, grad_ref, part_ref, shard_ref, *scratch):
    def compute():
        dq = jnp.concatenate([dq0_ref[...], dq1_ref[...]], axis=1)
        dk = jnp.concatenate([dk0_ref[...], dk1_ref[...]], axis=1)
        part_ref[...] = dot_nt(dq, wq_ref[...]) + dot_nt(dk, wk_ref[...])

    scatter_beside(marks, grad_ref, shard_ref, *scratch, compute)


def reduce_beside(parts, w_q, w_k, grads, tile, marks):
    n_rows, cols = parts[0].shape
    dim = w_q.shape[0]
    total = grads.shape[0] * grads.shape[1]
    half = pl.BlockSpec((tile, cols), lambda i: (i, 0))
    weight = pl.BlockSpec((dim, dim), lambda i: (0, 0))
    shard = shard_shape(total, cols)
    return pl.pallas_call(
        functools.partial(reduce_kernel, marks),
        grid=(n_rows // tile,),
        in_specs=[half] * 4 + [weight] * 2 + [pl.BlockSpec(memory_space=pl.ANY)],
        out_specs=[pl.BlockSpec((tile, dim), lambda i: (i, 0)), pl.BlockSpec(shard, lambda i: (0, 0, 0, 0))],
        out_shape=[jax.ShapeDtypeStruct((n_rows, dim), F32), jax.ShapeDtypeStruct(shard, F32)],
        scratch_shapes=scatter_scratch(total, cols),
        compiler_params=pltpu.CompilerParams(collective_id=0, has_side_effects=True),
        cost_estimate=pl.CostEstimate(flops=4 * n_rows * dim * dim, bytes_accessed=8 * n_rows * dim, transcendentals=0),
        name="reduce_beside",
    )(*parts, w_q, w_k, grads.reshape(total, cols))


def shard_spec(shards, slot, rows, block_of):
    per_piece = shards.shape[3] // rows

    def index(i):
        block = block_of(i)
        piece = block // per_piece
        part, hi, lo = piece // 4, (piece // 2) % 2, piece % 2
        x = hi + part * (lo - hi)
        y = lo + part * (hi - lo)
        return (y * 2 + x) * 2 + slot % 2, slot // 2, part, block % per_piece, 0

    return pl.BlockSpec((1, 1, 1, rows, shards.shape[4]), index)


def grad_specs(rows, cols, group):
    down = cols // rows
    return [pl.BlockSpec((rows, cols), lambda i: (i, group))] * 3 + [pl.BlockSpec((rows, cols), lambda i: (group * down + i % down, i // down))]


def out_kernel(o0_ref, o1_ref, dv0_ref, dv1_ref, part_ref, wo_ref, wv_ref, s0_ref, s1_ref, s2_ref, s3_ref, y_ref, dx_ref, gq_ref, gk_ref, gv_ref, go_ref):
    y_ref[...] = dot_nn(jnp.concatenate([o0_ref[...], o1_ref[...]], axis=1), wo_ref[...]).astype(BF16)
    dv = jnp.concatenate([dv0_ref[...], dv1_ref[...]], axis=1)
    dx_ref[...] = (part_ref[...] + dot_nt(dv, wv_ref[...])).astype(BF16)
    for src, dst in ((s0_ref, gq_ref), (s1_ref, gk_ref), (s2_ref, gv_ref), (s3_ref, go_ref)):
        dst[...] = src[0, 0, 0]


def back_project(parts, partial, w_o, w_v, gathered, tile):
    n_rows, cols = parts[0].shape
    dim = w_o.shape[1]
    steps = n_rows // tile
    piece = dim // steps
    half = pl.BlockSpec((tile, cols), lambda i: (i, 0))
    weight = pl.BlockSpec((dim, dim), lambda i: (0, 0))
    row_out = pl.BlockSpec((tile, dim), lambda i: (i, 0))
    return pl.pallas_call(
        out_kernel,
        grid=(steps,),
        in_specs=[half] * 4 + [row_out] + [weight] * 2 + [shard_spec(gathered, slot, piece, lambda i: i) for slot in range(4)],
        out_specs=[row_out] * 2 + grad_specs(piece, cols, 0),
        out_shape=[jax.ShapeDtypeStruct((n_rows, dim), BF16)] * 2 + [jax.ShapeDtypeStruct((dim, dim), F32)] * 4,
        cost_estimate=pl.CostEstimate(flops=4 * n_rows * dim * dim, bytes_accessed=12 * n_rows * dim, transcendentals=0),
        name="back_project",
    )(*parts, partial, w_o, w_v, *[gathered] * 4)


PLACE_PARTS = 2


def place_kernel(*refs):
    shards, outs = refs[:4 * PLACE_PARTS], refs[4 * PLACE_PARTS + 4:]
    rows = shards[0].shape[3]
    for i, shard in enumerate(shards):
        there = (i % PLACE_PARTS) * rows
        outs[i // PLACE_PARTS][there:there + rows] = shard[0, 0, 0]


def place(gathered, grads):
    piece, cols = gathered.shape[3:]
    sources = [shard_spec(gathered, slot, piece, lambda i, r=r: i * PLACE_PARTS + r) for slot in range(4) for r in range(PLACE_PARTS)]
    return pl.pallas_call(
        place_kernel,
        grid=(8 // PLACE_PARTS,),
        in_specs=sources + [pl.BlockSpec(memory_space=pl.ANY)] * 4,
        out_specs=grad_specs(PLACE_PARTS * piece, cols, 1),
        out_shape=[jax.ShapeDtypeStruct(g.shape, g.dtype) for g in grads],
        input_output_aliases={len(sources) + i: i for i in range(4)},
        cost_estimate=pl.CostEstimate(flops=0, bytes_accessed=8 * gathered.size, transcendentals=0),
        name="place",
    )(*[gathered] * len(sources), *grads)


def solution(mesh):
    n_seq = mesh.shape["sp"]
    row_spec = P(("dp", "sp"), None)
    grad_spec = P("dp", None)

    def local_layer(tokens, w_q, w_k, w_v, w_o, grad_y):
        scale = 1.0 / math.sqrt(tokens.shape[0] * n_seq * HEAD_DIM)
        projected = [project(tokens, grad_y, w_q, w_k, w_v, w_o, g, 1024) for g in range(GROUPS)]
        gathered = [lax.all_gather(p[4], "sp") for p in projected]
        parts = [None] * GROUPS
        parts[0] = attend(*projected[0][:4], gathered[0], scale, 0, 512)
        first = weight_grads(tokens, grad_y, *parts[0], 0, 1024)
        *parts[1], shard0 = attend(*projected[1][:4], gathered[1], scale, 1, 512, first, MARKS)
        shards0 = lax.all_gather(shard0, "sp")
        second = weight_grads(tokens, grad_y, *parts[1], 1, 1024)
        o, dq, dk, dv = zip(*parts)
        partial, shard1 = reduce_beside(dq + dk, w_q, w_k, second, 512, MARKS)
        shards1 = lax.all_gather(shard1, "sp")
        out_y, grad_x, *grads = back_project(o + dv, partial, w_o, w_v, shards0, 512)
        return (out_y, grad_x) + tuple(place(shards1, grads))

    return jax.shard_map(local_layer, mesh=mesh, in_specs=(row_spec, P(), P(), P(), P(), row_spec), out_specs=(row_spec, row_spec, grad_spec, grad_spec, grad_spec, grad_spec), check_vma=False)
```
